32 devices in a mesh: dp: 4 (over z), vocab: 8 (over y, x, core).
Axes of the slice: x: 2, y: 2, z: 4, core: 2. Of those that a mesh axis runs over, the one named last changes fastest.
Arguments:
- hidden: bfloat16 [32, 14, 4096], P('dp', None, 'vocab'), may hold values from -400 to 400
- weight: bfloat16 [4096, 16032], P(None, ('dp', 'vocab')), may hold values from -0.09375 to 0.09375
- targets: int32 [32, 14], P('dp'), may hold values from 0 to 16031
- lengths: int32 [4, 8], P('dp'), may hold values from 1 to 14, 56 in all within a row
- rewards: int32 [4, 8], P('dp'), may hold values from -256 to 256
- arrival: int32 [32], replicated, may hold values from 0 to 31, each once
Outputs:
- token_logprobs: float32 [32, 14], P('dp')
- advantages: float32 [32], P('dp')
- weighted: float32 [32], P('dp')
The draws below stay inside these ranges and needn't reach their ends.
Inputs may be any that keep to these rules, and one draw needn't show every extreme that they name: The lengths of one device's 8 completions sum to exactly 56, and one of them is 14. `arrival`: every completion number appears once; completion p * 8 + j is sample j of prompt p.
All inputs are finite; a program needn't handle non-finite values.
Results may differ from the reference program's by a relative error of at most 0.0003.
Values may be sent and summed in bfloat16 or wider, within the bound.
A program may use at most 192 MiB of HBM per device.

```python
import math
import jax
import jax.numpy as jnp
import numpy as np
from jax import lax

D = 4096
SAMPLES = 8
BLOCK = 14
CPL_DEV = 8
LIVE_DEV = 56
COMPL = 32
ROWS = 448
VOCAB = 16032
N_DP = 4


def draw_hidden(key, part):
    first = jax.random.fold_in(key, 0)
    base = jnp.clip(jax.random.normal(first, (COMPL, BLOCK, D), jnp.float32), -6.0, 6.0)
    factor = 3.0
    return (base * factor).astype(jnp.bfloat16)


def with_ends(values, rng, low, largest):
    shape = values.shape
    index_at = [jax.random.randint(jax.random.fold_in(rng, axis), (), 0, shape[axis]) for axis in range(len(shape))]
    values = values.at[tuple(index_at)].set(low)
    longest = shape.index(max(shape))
    index_at[longest] = (index_at[longest] + 1) % shape[longest]
    return values.at[tuple(index_at)].set(largest)


def levels(rng, extent, cuts, smallest, top_value):
    def one(position, parts):
        heights = jax.random.uniform(jax.random.fold_in(jax.random.fold_in(rng, 6), position), (parts,), jnp.float32, smallest / len(cuts), top_value / len(cuts))
        return jnp.repeat(jnp.exp(heights), extent[position] // parts).reshape((-1,) + (1,) * (len(extent) - position - 1))

    loudness = one(*cuts[0])
    for cut in cuts[1:]:
        loudness = loudness * one(*cut)
    return loudness


def profile(number_of, total, limit, skew):
    portions = [(1 << 20) // math.isqrt(standing ** skew) + 1 for standing in range(2, number_of + 1)]
    rest, given = total - limit - (number_of - 1), [1] * (number_of - 1)
    while rest > 0:
        free = [i for i in range(number_of - 1) if given[i] < limit]
        pool, budget = sum([portions[i] for i in free]), rest
        for i in free:
            extra = min(limit - given[i], max(1, budget * portions[i] // pool), rest)
            given[i] = given[i] + extra
            rest = rest - extra
    return np.array([limit] + given)


def ragged_sizes(rng, count, total, bound, lean):
    if count == 2:
        one = jax.random.randint(rng, (), max(1, total - bound), min(bound, total - 1) + 1)
        return jnp.stack([one, total - one])
    sizes = jnp.asarray(profile(count, total, bound, lean), jnp.int32)
    pairs = (count - 1) // 2
    donor, sink = sizes[1:1 + 2 * pairs:2], sizes[2:2 + 2 * pairs:2]
    slack = jnp.minimum(donor - 1, bound - sink)
    shifted = jax.random.randint(jax.random.fold_in(rng, 1), (pairs,), 0, 1 << 20) % (slack + 1)
    sizes = sizes.at[1:1 + 2 * pairs:2].set(donor - shifted).at[2:2 + 2 * pairs:2].set(sink + shifted)
    return sizes[jax.random.permutation(jax.random.fold_in(rng, 2), count)]


def centred(stream_key, shape, scale, limit, cuts=(), held_as=jnp.bfloat16):
    level = levels(stream_key, shape, cuts, -0.22, 0.18) if cuts else 1.0
    drawn = jax.random.normal(stream_key, shape, jnp.float32) * scale * level
    return jnp.minimum(jnp.maximum(drawn, -limit), limit).astype(held_as)


def setup_inputs(seed: int = 0) -> dict:
    splits = jax.random.split(jax.random.key(seed), 7)
    return {
        "hidden": draw_hidden(jax.random.fold_in(splits[6], 71), 0),
        "weight": centred(splits[1], (D, VOCAB), D ** -0.5, 0.09375, ((1, 32),)),
        "targets": with_ends(jax.random.randint(splits[2], (COMPL, BLOCK), 0, VOCAB), jax.random.fold_in(splits[2], 1), 0, VOCAB - 1).astype(jnp.int32),
        "lengths": jax.vmap(lambda own: ragged_sizes(own, CPL_DEV, LIVE_DEV, BLOCK, 2))(jax.random.split(splits[3], N_DP)).reshape((N_DP, CPL_DEV)).astype(jnp.int32),
        "rewards": with_ends(jax.random.randint(splits[4], (N_DP, CPL_DEV), -256, 257), jax.random.fold_in(splits[4], 1), -256, 256).astype(jnp.int32),
        "arrival": jax.random.permutation(splits[5], COMPL).astype(jnp.int32),
    }


reward_unit = 1.0 / 64.0


def reference(hidden, weight, targets, lengths, rewards, arrival):
    row_states = hidden.reshape(ROWS, D)
    token_ids = targets.reshape(ROWS)
    column_span = VOCAB // N_DP

    def absorb(carried, block_index):
        highest, totals = carried
        columns = lax.dynamic_slice_in_dim(weight, block_index * column_span, column_span, 1)
        logits = jnp.dot(row_states, columns, preferred_element_type=jnp.float32)
        block_high = jnp.max(logits, axis=1)
        block_total = jnp.sum(jnp.exp(logits - block_high[:, None]), axis=1)
        joined = jnp.maximum(highest, block_high)
        totals = totals * jnp.exp(highest - joined) + block_total * jnp.exp(block_high - joined)
        return (joined, totals), None

    start = (jnp.full((ROWS,), -1e30, jnp.float32), jnp.zeros((ROWS,), jnp.float32))
    (highest, totals), _ = lax.scan(absorb, start, jnp.arange(N_DP, dtype=jnp.int32))
    chosen = jnp.take(weight, token_ids, axis=1)
    picked = jnp.sum(row_states.astype(jnp.float32) * chosen.T.astype(jnp.float32), axis=1)
    slot_lengths = lengths.reshape(COMPL)
    usable = jnp.arange(BLOCK, dtype=jnp.int32)[None, :] < slot_lengths[:, None]
    slot_logprob = jnp.where(usable, (picked - highest - jnp.log(totals)).reshape(COMPL, BLOCK), 0.0)
    token_logprobs = jnp.zeros((COMPL, BLOCK), jnp.float32).at[arrival].set(slot_logprob)
    reward = jnp.zeros((COMPL,), jnp.float32).at[arrival].set(rewards.reshape(COMPL).astype(jnp.float32) * reward_unit)
    length = jnp.zeros((COMPL,), jnp.float32).at[arrival].set(slot_lengths.astype(jnp.float32))
    group = jnp.sum(reward.reshape(COMPL // SAMPLES, SAMPLES), axis=1)
    advantages = reward - (jnp.repeat(group, SAMPLES) - reward) / (SAMPLES - 1.0)
    weighted = advantages * jnp.sum(token_logprobs, axis=1) / length
    return token_logprobs, advantages, weighted
```

```python
import functools

import jax
import jax.numpy as jnp
from jax import lax
from jax.experimental import pallas as pl
from jax.experimental.pallas import tpu as pltpu
from jax.sharding import PartitionSpec as P

SAMPLES = 8
LANES = 128
MESH = pl.DeviceIdType.MESH

reward_unit = 1.0 / 64.0


def flip(index, bit):
    return index + bit - 2 * bit * ((index // bit) % 2)


def flip_mask(index, mask):
    bit = 1
    while bit <= mask:
        if mask & bit:
            index = flip(index, bit)
        bit *= 2
    return index


def kernel(
    n_dp, n_v, group, live_pad,
    hid, w_hbm, tgt, lens, rews, arr,
    out_lp, out_adv, out_wt,
    xbuf, wbuf, hpad, tpad, meta, acc, st1, st2,
    wsem, psend, precv, msend, mrecv, s1send, s1recv, s2send, s2recv,
):
    z = lax.axis_index("dp")
    v = lax.axis_index("vocab")
    slots, window, feat = hid.shape
    width = w_hbm.shape[1]
    per_device = slots

    barrier = pltpu.get_barrier_semaphore()
    for k in range(1, n_dp):
        pl.semaphore_signal(barrier, inc=1, device_id={"dp": (z + k) % n_dp, "vocab": v}, device_id_type=MESH)
    for k in range(1, n_v):
        pl.semaphore_signal(barrier, inc=1, device_id={"dp": z, "vocab": (v + k) % n_v}, device_id_type=MESH)

    wcopy = pltpu.make_async_copy(w_hbm, wbuf, wsem)
    wcopy.start()

    lane = lax.broadcasted_iota(jnp.int32, (1, LANES), 1)
    lane_slot = lane // group
    lane_pos = lane % group
    dest = jnp.full((1, LANES), -1, jnp.int32)
    reward_row = jnp.zeros((1, LANES), jnp.int32)
    length_row = jnp.zeros((1, LANES), jnp.int32)
    comp_row = jnp.zeros((1, LANES), jnp.int32)
    offset = jnp.int32(0)
    for s in range(slots):
        length = lens[0, s]
        mine = lane_slot == s
        dest = jnp.where(mine & (lane_pos < length), offset + lane_pos, dest)
        reward_row = jnp.where(mine, rews[0, s], reward_row)
        length_row = jnp.where(mine, length, length_row)
        comp_row = jnp.where(mine, arr[z * slots + s], comp_row)
        offset = offset + length

    hpad[...] = jnp.zeros(hpad.shape, hpad.dtype)
    hpad[:, :window, :] = hid[...]
    row_ids = lax.broadcasted_iota(jnp.int32, (live_pad, LANES), 0)
    choose = jnp.where(row_ids == dest, 1.0, 0.0).astype(jnp.bfloat16)
    packed = jnp.dot(choose, hpad[...].reshape(slots * group, feat), preferred_element_type=jnp.float32)
    xbuf[v, z] = packed.astype(xbuf.dtype)

    tpad[...] = jnp.zeros(tpad.shape, tpad.dtype)
    tpad[:, :window] = tgt[...].astype(jnp.float32)
    spread = tpad[...]
    step = group
    while step < LANES:
        spread = spread + pltpu.roll(spread, step, 1)
        step *= 2
    sub8 = lax.broadcasted_iota(jnp.int32, (slots, LANES), 0)
    target_row = jnp.sum(jnp.where(sub8 == lane_slot, spread, 0.0), axis=0, keepdims=True)
    sub = lax.broadcasted_iota(jnp.int32, (8, LANES), 0)
    tile = jnp.where(sub == 0, dest.astype(jnp.float32), 0.0)
    tile = jnp.where(sub == 1, target_row, tile)
    tile = jnp.where(sub == 2, reward_row.astype(jnp.float32) * reward_unit, tile)
    tile = jnp.where(sub == 3, length_row.astype(jnp.float32), tile)
    tile = jnp.where(sub == 4, comp_row.astype(jnp.float32), tile)
    meta[z] = tile

    pl.semaphore_wait(barrier, n_dp - 1 + n_v - 1)

    sends = []

    def piece_to(vv, q, to_dp, to_v):
        copy = pltpu.make_async_remote_copy(
            src_ref=xbuf.at[vv, q], dst_ref=xbuf.at[vv, q],
            send_sem=psend.at[len(sends)], recv_sem=precv.at[vv, q],
            device_id={"dp": to_dp, "vocab": to_v}, device_id_type=MESH,
        )
        copy.start()
        sends.append(copy)

    def piece_wait(vv, q):
        pltpu.make_async_remote_copy(
            src_ref=xbuf.at[vv, q], dst_ref=xbuf.at[vv, q],
            send_sem=psend.at[0], recv_sem=precv.at[vv, q],
            device_id={"dp": z, "vocab": v}, device_id_type=MESH,
        ).wait_recv()

    if n_dp & (n_dp - 1) == 0:
        order = [flip_mask(z, k) for k in range(n_dp)]
    else:
        order = [(z + k) % n_dp for k in range(n_dp)]
    sib = flip(v, 1)
    xn = flip(v, 2)
    yn = flip(v, 4)
    diag = flip(xn, 4)

    for k in range(1, n_dp):
        piece_to(v, z, order[k], v)
    piece_to(v, z, z, xn)
    piece_to(v, z, z, yn)
    piece_to(v, z, z, sib)

    metas = []
    for k in range(1, n_dp):
        copy = pltpu.make_async_remote_copy(
            src_ref=meta.at[z], dst_ref=meta.at[z], send_sem=msend.at[k], recv_sem=mrecv.at[k],
            device_id={"dp": (z + k) % n_dp, "vocab": v}, device_id_type=MESH,
        )
        copy.start()
        metas.append(copy)

    def handle_near(k):
        q = order[k]
        piece_wait(xn, q)
        if k % 2 == 0:
            piece_to(xn, q, z, yn)
        piece_to(xn, q, z, sib)
        piece_wait(yn, q)
        if k % 2 == 1:
            piece_to(yn, q, z, xn)
        piece_to(yn, q, z, sib)

    def handle_diag(k):
        q = order[k]
        piece_wait(diag, q)
        piece_to(diag, q, z, sib)

    def dot(vv, first):
        rows = xbuf[vv].reshape(n_dp * live_pad, feat)
        part = jnp.dot(rows, wbuf[pl.ds(pl.multiple_of(vv * feat, feat), feat), :], preferred_element_type=jnp.float32)
        if first:
            acc[...] = part
        else:
            acc[...] += part

    for k in range(1, n_dp):
        q = order[k]
        piece_wait(v, q)
        piece_to(v, q, z, xn)
        piece_to(v, q, z, yn)
        piece_to(v, q, z, sib)
        handle_near(k - 1)
        if k >= 2:
            handle_diag(k - 2)
    wcopy.wait()
    dot(v, True)
    handle_near(n_dp - 1)
    if n_dp >= 2:
        handle_diag(n_dp - 2)
    for k in range(n_dp):
        piece_wait(sib, order[k])
    dot(sib, False)
    handle_diag(n_dp - 1)
    dot(xn, False)
    dot(yn, False)
    for other in (flip(xn, 1), flip(yn, 1)):
        for k in range(n_dp):
            piece_wait(other, order[k])
        dot(other, False)
    dot(diag, False)
    other = flip(diag, 1)
    for k in range(n_dp):
        piece_wait(other, order[k])
    dot(other, False)

    for k in range(1, n_dp):
        pltpu.make_async_remote_copy(
            src_ref=meta.at[z], dst_ref=meta.at[(z + n_dp - k) % n_dp], send_sem=msend.at[k], recv_sem=mrecv.at[k],
            device_id={"dp": z, "vocab": v}, device_id_type=MESH,
        ).wait_recv()

    first_column = ((z * n_v + v) * width).astype(jnp.float32)
    column_ids = lax.broadcasted_iota(jnp.int32, (live_pad, width), 1).astype(jnp.float32)
    row_f = row_ids.astype(jnp.float32)
    for q in range(n_dp):
        dest_q = meta[q, 0:1, :]
        target_q = meta[q, 1:2, :]
        hit = row_f == dest_q
        target_col = jnp.sum(jnp.where(hit, target_q, 0.0), axis=1, keepdims=True) - first_column
        logits = acc[q * live_pad:(q + 1) * live_pad, :]
        highest = jnp.max(logits, axis=1, keepdims=True)
        totals = jnp.sum(jnp.exp(logits - highest), axis=1, keepdims=True)
        picked = jnp.sum(jnp.where(column_ids == target_col, logits, 0.0), axis=1, keepdims=True)
        st1[v, 0, q:q + 1, :] = jnp.sum(jnp.where(hit, highest, 0.0), axis=0, keepdims=True)
        st1[v, 1, q:q + 1, :] = jnp.sum(jnp.where(hit, totals, 0.0), axis=0, keepdims=True)
        st1[v, 2, q:q + 1, :] = jnp.sum(jnp.where(hit, picked, 0.0), axis=0, keepdims=True)

    def exchange(buf, me, count, send, recv, target):
        out = []
        for k in range(1, count):
            copy = pltpu.make_async_remote_copy(
                src_ref=buf.at[me], dst_ref=buf.at[me], send_sem=send.at[k], recv_sem=recv.at[k],
                device_id=target((me + k) % count), device_id_type=MESH,
            )
            copy.start()
            out.append(copy)
        for k in range(1, count):
            pltpu.make_async_remote_copy(
                src_ref=buf.at[me], dst_ref=buf.at[(me + count - k) % count], send_sem=send.at[k], recv_sem=recv.at[k],
                device_id=target(me), device_id_type=MESH,
            ).wait_recv()
        return out

    def merged(buf, count):
        highest = buf[0, 0]
        for k in range(1, count):
            highest = jnp.maximum(highest, buf[k, 0])
        totals = jnp.zeros_like(highest)
        picked = jnp.zeros_like(highest)
        for k in range(count):
            totals = totals + buf[k, 1] * jnp.exp(buf[k, 0] - highest)
            picked = picked + buf[k, 2]
        return highest, totals, picked

    pending = exchange(st1, v, n_v, s1send, s1recv, lambda i: {"dp": z, "vocab": i})
    highest, totals, picked = merged(st1, n_v)
    st2[z, 0] = highest
    st2[z, 1] = totals
    st2[z, 2] = picked
    pending += exchange(st2, z, n_dp, s2send, s2recv, lambda i: {"dp": i, "vocab": v})
    highest, totals, picked = merged(st2, n_dp)

    valid = meta[:, 0, :] >= 0.0
    logprob = jnp.where(valid, picked - highest - jnp.log(totals), 0.0)
    comp = meta[:, 4, :]
    reward_all = meta[:, 2, :]
    length_all = meta[:, 3, :]
    first_comp = (z * per_device).astype(jnp.float32)
    sub_out = lax.broadcasted_iota(jnp.int32, (per_device, LANES), 0)

    def fold(x):
        step = group
        while step < LANES:
            x = x + pltpu.roll(x, step, 1)
            step *= 2
        return x

    lp = jnp.zeros((per_device, LANES), jnp.float32)
    rw = lp
    ln = lp
    for i in range(per_device):
        own = comp == first_comp + i
        lp = jnp.where(sub_out == i, jnp.sum(jnp.where(own, logprob, 0.0), axis=0, keepdims=True), lp)
        rw = jnp.where(sub_out == i, jnp.sum(jnp.where(own, reward_all, 0.0), axis=0, keepdims=True), rw)
        ln = jnp.where(sub_out == i, jnp.sum(jnp.where(own, length_all, 0.0), axis=0, keepdims=True), ln)
    total_lp = jnp.sum(lp, axis=1, keepdims=True)
    lp, rw, ln = fold(lp), fold(rw), fold(ln)
    out_lp[...] = lp[:, :window]
    adv_rows = jnp.zeros((per_device, LANES), jnp.float32)
    for g in range(per_device // SAMPLES):
        inside = (sub_out >= g * SAMPLES) & (sub_out < (g + 1) * SAMPLES)
        total = jnp.sum(jnp.where(inside, rw, 0.0), axis=0, keepdims=True)
        adv_rows = jnp.where(inside, rw - (total - rw) / (SAMPLES - 1.0), adv_rows)
    wt_rows = adv_rows * total_lp / ln
    lane_out = lax.broadcasted_iota(jnp.int32, (per_device, LANES), 1)
    diag_mask = lane_out == sub_out
    out_adv[...] = jnp.sum(jnp.where(diag_mask, adv_rows, 0.0), axis=0, keepdims=True)[:, :per_device]
    out_wt[...] = jnp.sum(jnp.where(diag_mask, wt_rows, 0.0), axis=0, keepdims=True)[:, :per_device]

    for copy in sends + metas + pending:
        copy.wait_send()


def live_rows(lengths_total):
    return (lengths_total + 15) // 16 * 16


def local(n_dp, n_v, hidden, weight, targets, lengths, rewards, arrival):
    slots, window, feat = hidden.shape
    group = LANES // slots
    live = slots * window // 2
    live_pad = live_rows(live)
    vmem = pl.BlockSpec(memory_space=pltpu.VMEM)
    smem = pl.BlockSpec(memory_space=pltpu.SMEM)
    n_sends = (n_dp - 1) + 3 + 3 * (n_dp - 1) + 4 * n_dp
    dma = pltpu.SemaphoreType.DMA
    lp, adv, wt = pl.pallas_call(
        functools.partial(kernel, n_dp, n_v, group, live_pad),
        out_shape=(
            jax.ShapeDtypeStruct((slots, window), jnp.float32),
            jax.ShapeDtypeStruct((1, slots), jnp.float32),
            jax.ShapeDtypeStruct((1, slots), jnp.float32),
        ),
        in_specs=[vmem, pl.BlockSpec(memory_space=pl.ANY), vmem, smem, smem, smem],
        out_specs=(vmem, vmem, vmem),
        scratch_shapes=[
            pltpu.VMEM((n_v, n_dp, live_pad, feat), jnp.bfloat16),
            pltpu.VMEM(weight.shape, jnp.bfloat16),
            pltpu.VMEM((slots, group, feat), jnp.bfloat16),
            pltpu.VMEM((slots, LANES), jnp.float32),
            pltpu.VMEM((n_dp, 8, LANES), jnp.float32),
            pltpu.VMEM((n_dp * live_pad, weight.shape[1]), jnp.float32),
            pltpu.VMEM((n_v, 3, n_dp, LANES), jnp.float32),
            pltpu.VMEM((n_dp, 3, n_dp, LANES), jnp.float32),
            dma,
            dma((n_sends + n_dp,)),
            dma((n_v, n_dp)),
            dma((n_dp,)),
            dma((n_dp,)),
            dma((n_v,)),
            dma((n_v,)),
            dma((n_dp,)),
            dma((n_dp,)),
        ],
        compiler_params=pltpu.CompilerParams(
            collective_id=0, has_side_effects=True, vmem_limit_bytes=60000 * 1024
        ),
    )(hidden, weight, targets, lengths, rewards, arrival)
    return lp, adv.reshape(slots), wt.reshape(slots)


def solution(mesh):
    return jax.shard_map(
        functools.partial(local, mesh.shape["dp"], mesh.shape["vocab"]),
        mesh=mesh,
        in_specs=(
            P("dp", None, "vocab"),
            P(None, ("dp", "vocab")),
            P("dp", None),
            P("dp", None),
            P("dp", None),
            P(),
        ),
        out_specs=(P("dp", None), P("dp"), P("dp")),
        check_vma=False,
    )
```
